256 devices in a mesh: tm: 4 (over x), chan: 64 (over z, y, core).
Axes of the slice: x: 4, y: 4, z: 8, core: 2. Of those that a mesh axis runs over, the one named last changes fastest.
Arguments:
- voltages: bfloat16 [8, 4, 32768, 512], P(None, None, ('tm', 'chan')), may hold values from -6 to 6
- taps: float32 [4, 512], replicated, may hold values from -3 to 3
- busy_mask: int32 [512], replicated, may hold values from 0 to 1, as said below
- drift_low: int32 [512], replicated, may hold values from -16 to 1
Outputs:
- drift_power: float32 [8, 256, 16, 2048], P(None, 'chan', None, 'tm')
The draws below stay inside these ranges and needn't reach their ends.
Inputs may be any that keep to these rules, and one draw needn't show every extreme that they name: `busy_mask`: exactly 256 entries are 1.
All inputs are finite; a program needn't handle non-finite values.
Results may differ from the reference program's by a relative error of at most 0.008.
Values may be sent and summed in bfloat16 or wider, within the bound.
A program may use at most 128 MiB of HBM per device.

```python
import math
import jax
import jax.numpy as jnp
from jax import lax

COARSE_CHANNELS = 512
FINE = 2048
FA = 32
FB = 64
TAPS = 4
NDRIFT = 16
DSPAN = 16
FSTEP = 4
BEAMS = 8
SPEC = 32768
STEPS = 16
BUSY = 256
N_TM = 4


def draw_busy_mask(key, part):
    perm_key = jax.random.fold_in(key, 11)
    reward_key = jax.random.fold_in(key, 23)
    permuted_order = jax.random.permutation(perm_key, COARSE_CHANNELS).astype(jnp.int32)
    block_reward = jax.random.randint(reward_key, (COARSE_CHANNELS // 8,), 0, 4, dtype=jnp.int32)
    merit_scores = jnp.repeat(block_reward, 8, total_repeat_length=COARSE_CHANNELS) * (2 * COARSE_CHANNELS) + permuted_order
    chosen = lax.top_k(merit_scores, BUSY)[1]
    return jnp.zeros((COARSE_CHANNELS,), jnp.int32).at[chosen].set(1)


def set_ends(drawn, key, low, largest):
    longest = drawn.shape.index(max(drawn.shape))
    spots = []
    for shift in (0, 1):
        where = [jax.random.randint(jax.random.fold_in(key, axis), (), 0, length) for axis, length in enumerate(drawn.shape)]
        where[longest] = (where[longest] + shift) % drawn.shape[longest]
        spots.append(tuple(where))
    return drawn.at[spots[0]].set(low).at[spots[1]].set(largest)


def levels(own_key, extent, cuts, least, high):
    def one(axis_at, shards_of):
        draws = jax.random.uniform(jax.random.fold_in(jax.random.fold_in(own_key, 6), axis_at), (shards_of,), jnp.float32, least / len(cuts), high / len(cuts))
        return jnp.repeat(jnp.exp(draws), extent[axis_at] // shards_of).reshape((-1,) + (1,) * (len(extent) - axis_at - 1))

    factor_of = one(*cuts[0])
    for cut in cuts[1:]:
        factor_of = factor_of * one(*cut)
    return factor_of


def noise(key, dims, spread, most, shards=(), kind=jnp.bfloat16):
    level = levels(key, dims, shards, -0.22, 0.18) if shards else 1.0
    values = jax.random.normal(key, dims, jnp.float32) * spread * level
    return jnp.minimum(jnp.maximum(values, -most), most).astype(kind)


def setup_inputs(seed: int = 0) -> dict:
    keys = jax.random.split(jax.random.key(seed), 5)
    return {
        "voltages": noise(keys[0], (BEAMS, 4, SPEC, COARSE_CHANNELS), 1.0, 6.0, ((2, 256),)),
        "taps": noise(keys[1], (TAPS, COARSE_CHANNELS), 0.5, 3.0, (), jnp.float32),
        "busy_mask": draw_busy_mask(jax.random.fold_in(keys[4], 71), 0),
        "drift_low": set_ends(jax.random.randint(keys[3], (COARSE_CHANNELS,), -DSPAN, DSPAN - NDRIFT + 2), jax.random.fold_in(keys[3], 1), -DSPAN, (DSPAN - NDRIFT + 2) - 1).astype(jnp.int32),
    }


def busy_index(busy_mask, busy_count):
    mask_ints = busy_mask.astype(jnp.int32)
    before = (jnp.cumsum(mask_ints) - mask_ints).astype(jnp.int32)
    slot_ids = jnp.arange(busy_count, dtype=jnp.int32)
    is_slot = (mask_ints[:, None] == 1) & (before[:, None] == slot_ids[None, :])
    positions = jnp.arange(busy_mask.shape[0], dtype=jnp.int32)
    return jnp.sum(jnp.where(is_slot, positions[:, None], 0), axis=0).astype(jnp.int32)


def real_dft(sample_pos, freq_ids, length):
    phase_index = (sample_pos[:, None] * freq_ids[None, :]) % length
    angles = phase_index.astype(jnp.float32) * (2.0 * math.pi / length)
    cosines = jnp.cos(angles)
    sine_table = jnp.sin(angles)
    upper = jnp.stack([cosines, -sine_table], axis=1)
    lower = jnp.stack([sine_table, cosines], axis=1)
    return jnp.stack([upper, lower], axis=0).astype(jnp.bfloat16)


def to_bfloat(values):
    return lax.optimization_barrier(values.astype(jnp.bfloat16)).astype(jnp.float32)


def detect_power(spectra):
    items, lanes, chan_rows, samples = spectra.shape
    step_count = samples // (FA * FB)
    shaped = spectra.reshape(items, 2, 2, chan_rows, step_count, FA, FB).astype(jnp.float32)
    short_ids = jnp.arange(FA, dtype=jnp.int32)
    long_ids = jnp.arange(FB, dtype=jnp.int32)
    first_dft = real_dft(short_ids, short_ids, FA).astype(jnp.float32)
    second_dft = real_dft(long_ids, long_ids, FB).astype(jnp.float32)
    first_pass = jnp.einsum("xopctab,paqf->xoqctfb", shaped, first_dft, precision=lax.Precision.HIGHEST)
    twist = (short_ids[:, None] * long_ids[None, :]) % (FA * FB)
    twist_angles = twist.astype(jnp.float32) * (2.0 * math.pi / (FA * FB))
    twist_cos = jnp.cos(twist_angles)
    twist_sin = jnp.sin(twist_angles)
    real_part = first_pass[:, :, 0]
    imag_part = first_pass[:, :, 1]
    turned = jnp.stack([real_part * twist_cos + imag_part * twist_sin, imag_part * twist_cos - real_part * twist_sin], axis=2).astype(jnp.bfloat16)
    second_pass = jnp.einsum("xoqctfb,qbsg->xosctgf", turned.astype(jnp.float32), second_dft, precision=lax.Precision.HIGHEST)
    powers = jnp.sum(second_pass * second_pass, axis=(1, 2)) / (4.0 * FA * FB)
    return powers.reshape(items, chan_rows, step_count, FA * FB)


def drift_rows(step_rows, first_step, drift_rates, first_bin, bin_width, pad_width):
    padded = jnp.pad(step_rows, ((0, 0), (0, 0), (0, 0), (pad_width, pad_width)))
    chan_rows = step_rows.shape[1]
    chan_pick = jnp.arange(chan_rows, dtype=jnp.int32)[:, None, None]
    start_offsets = jnp.arange(bin_width, dtype=jnp.int32)
    running = jnp.zeros((step_rows.shape[0], chan_rows, drift_rates.shape[1], bin_width), jnp.float32)
    for row_index in range(step_rows.shape[2]):
        step_time = first_step + row_index
        anchor = pad_width + first_bin + drift_rates * step_time
        positions = (anchor[:, :, None] + start_offsets[None, None, :]).astype(jnp.int32)
        picked = padded[:, :, row_index][:, chan_pick, positions]
        running = running + picked
    return running


def reference(voltages, taps, busy_mask, drift_low):
    slot_index = busy_index(busy_mask, BUSY)
    coarse_dft = real_dft(jnp.arange(COARSE_CHANNELS, dtype=jnp.int32), slot_index, COARSE_CHANNELS).astype(jnp.float32)

    def one_beam(beam_volts):
        extended = jnp.pad(beam_volts, ((0, 0), (0, TAPS - 1), (0, 0)))
        filtered = taps[0] * extended[:, 0:SPEC]
        for tap_index in range(1, TAPS):
            filtered = filtered + taps[tap_index] * extended[:, tap_index:tap_index + SPEC]
        filtered = filtered.astype(jnp.bfloat16).astype(jnp.float32).reshape(2, 2, SPEC, COARSE_CHANNELS)
        coarse = jnp.einsum("opsn,pnqr->oqrs", filtered, coarse_dft, precision=lax.Precision.HIGHEST)
        coarse = (coarse * COARSE_CHANNELS ** -0.5).astype(jnp.bfloat16)
        return detect_power(coarse.reshape(1, 4, BUSY, SPEC))[0]

    powers = lax.map(one_beam, voltages)
    low_rates = drift_low[slot_index].astype(jnp.int32)
    drift_rates = (low_rates[:, None] + jnp.arange(NDRIFT, dtype=jnp.int32)[None, :]).astype(jnp.int32)
    pad_width = DSPAN * (STEPS - 1)
    drift_total = jnp.zeros((BEAMS, BUSY, NDRIFT, FINE), jnp.float32)
    for group_index in range(N_TM):
        step_rows = powers[:, :, group_index * FSTEP:(group_index + 1) * FSTEP]
        drift_total = drift_total + to_bfloat(drift_rows(step_rows, group_index * FSTEP, drift_rates, 0, FINE, pad_width))
    return drift_total / STEPS
```

```python
import functools
import math

import jax
import jax.numpy as jnp
import numpy as np
from jax import lax
from jax.experimental import pallas as pl
from jax.experimental.pallas import tpu as pltpu
from jax.sharding import PartitionSpec as P

TAPS = 4
NDRIFT = 16
SRC = 16
SEG = 128
FINE = SRC * SEG
HALO = 8
BINS = 512
WIN = BINS // SEG + 2
PAD = 2
BLOCKS = PAD + SRC + 6
STRIDE = 72
VMEM_LIMIT = 60 * 1024 * 1024


def coarse_table(channels):
    n = np.arange(channels, dtype=np.int64)
    angle = ((n[:, None] * n[None, :]) % channels) * (2.0 * math.pi / channels)
    cos, sin = np.cos(angle), np.sin(angle)
    table = np.concatenate([cos, sin, -sin, cos], axis=1)
    return jnp.asarray(table.astype(np.float32)).astype(jnp.bfloat16)


def segment_table():
    s = np.arange(SEG, dtype=np.int64)
    lane = np.arange(SEG, dtype=np.int64)
    g = (lane % 16) * 8 + lane // 16
    angle = ((s[:, None] * g[None, :]) % SEG) * (2.0 * math.pi / SEG)
    cos, sin = np.cos(angle), np.sin(angle)
    table = np.concatenate(
        [np.concatenate([cos, -sin], axis=1), np.concatenate([sin, cos], axis=1)], axis=0
    )
    return jnp.asarray(table.astype(np.float32)).astype(jnp.bfloat16)


def twist_table():
    f = np.arange(SRC, dtype=np.int64)
    s = np.arange(SEG, dtype=np.int64)
    angle = ((f[:, None] * s[None, :]) % FINE) * (2.0 * math.pi / FINE)
    return jnp.asarray(np.stack([np.cos(angle), np.sin(angle)]).astype(np.float32))


def quarter_turns(value, count):
    re, im = value
    count %= 4
    if count == 0:
        return re, im
    if count == 1:
        return im, -re
    if count == 2:
        return -re, -im
    return -im, re


def turned_by(value, cos, sin):
    re, im = value
    return re * cos + im * sin, im * cos - re * sin


def added(left, right):
    return left[0] + right[0], left[1] + right[1]


def dropped(left, right):
    return left[0] - right[0], left[1] - right[1]


def dft4(values):
    a = added(values[0], values[2])
    b = dropped(values[0], values[2])
    c = added(values[1], values[3])
    d = quarter_turns(dropped(values[1], values[3]), 1)
    return [added(a, c), added(b, d), dropped(a, c), dropped(b, d)]


def filter_beam(volt, halo, taps_ref, ext, filt):
    tiles = ext.shape[0]
    for entry in range(4):
        o, p = entry // 2, entry % 2
        rows = volt(entry).astype(jnp.float32)
        tail = halo(entry).astype(jnp.float32)
        for l in range(tiles):
            lanes = slice(l * 128, (l + 1) * 128)
            ext[l, 0:SEG, :] = rows[:, lanes]
            ext[l, SEG : SEG + HALO, :] = tail[:, lanes]
        for l in range(tiles):
            lanes = slice(l * 128, (l + 1) * 128)
            total = taps_ref[0:1, lanes] * ext[l, 0:SEG, :]
            for tap in range(1, TAPS):
                total = total + taps_ref[tap : tap + 1, lanes] * ext[l, tap : tap + SEG, :]
            column = (p * tiles + l) * 128
            filt[o * SEG : (o + 1) * SEG, column : column + 128] = total.astype(jnp.bfloat16)


def coarse_of(filt, dft_ref, q, scale):
    depth = filt.shape[1]
    weights = dft_ref[:, q * depth : (q + 1) * depth]
    out = lax.dot_general(
        weights, filt[...], (((1,), (1,)), ((), ())), preferred_element_type=jnp.float32
    )
    return (out * scale).astype(jnp.bfloat16)


def coarse_kernel(volt_ref, halo_ref, taps_ref, dft_ref, out_ref, ext, filt):
    filter_beam(lambda i: volt_ref[0, i], lambda i: halo_ref[0, i], taps_ref, ext, filt)
    scale = taps_ref.shape[1] ** -0.5
    for q in range(2):
        block = coarse_of(filt, dft_ref, q, scale)
        for d in range(SRC):
            for o in range(2):
                out_ref[d, 0, o, q] = block[d * 16 : (d + 1) * 16, o * SEG : (o + 1) * SEG]


def fine_beam(load, twist_ref, seg_ref, turned, spread, beam):
    for o in range(2):
        inner = []
        for b in range(4):
            group = []
            for a in range(4):
                src = 4 * a + b
                group.append(
                    (load(src, o, 0).astype(jnp.float32), load(src, o, 1).astype(jnp.float32))
                )
            row = dft4(group)
            for f0 in range(1, 4):
                if b:
                    angle = 2.0 * math.pi * b * f0 / 16
                    row[f0] = turned_by(row[f0], math.cos(angle), math.sin(angle))
            inner.append(row)
        for f0 in range(4):
            outs = dft4([inner[b][f0] for b in range(4)])
            for f1 in range(4):
                f = f0 + 4 * f1
                value = outs[f1]
                if f:
                    value = turned_by(value, twist_ref[0, f : f + 1, :], twist_ref[1, f : f + 1, :])
                rows = slice((o * SRC + f) * 16, (o * SRC + f + 1) * 16)
                turned[rows, 0:SEG] = value[0].astype(jnp.bfloat16)
                turned[rows, SEG : 2 * SEG] = value[1].astype(jnp.bfloat16)
    lane = lax.broadcasted_iota(jnp.int32, (8, 128), 1)
    power = None
    for o in range(2):
        second = jnp.dot(
            turned[o * 256 : (o + 1) * 256, :], seg_ref[...], preferred_element_type=jnp.float32
        )
        re, im = second[:, 0:SEG], second[:, SEG : 2 * SEG]
        squares = re * re + im * im
        power = squares if power is None else power + squares
    power = power * (1.0 / (4.0 * FINE))
    for half in range(2):
        blocks = [power[f * 16 + half * 8 : f * 16 + half * 8 + 8, :] for f in range(SRC)]
        for bit in range(4):
            shift = 1 << bit
            upper = (lane & shift) != 0
            for f in range(SRC):
                if f & shift:
                    continue
                low, high = blocks[f], blocks[f | shift]
                blocks[f] = jnp.where(upper, pltpu.roll(high, shift, 1), low)
                blocks[f | shift] = jnp.where(upper, high, pltpu.roll(low, 128 - shift, 1))
        for h in range(SRC):
            spread[PAD + h, pl.ds(half * 64 + beam, 8, stride=8), :] = blocks[h]


def clear_pads(spread):
    zero = jnp.zeros((128, 128), jnp.float32)
    for h in range(PAD):
        spread[h] = zero
    for h in range(PAD + SRC, BLOCKS):
        spread[h] = zero


def shifted_windows(step, low_ref, spread, store):
    lane = lax.broadcasted_iota(jnp.int32, (8, 128), 1)
    count = 4 * 3 + WIN

    def windows(channel):
        start = low_ref[channel] * step + PAD * 128
        first = start // 128
        rest = start - first * 128
        rows = pl.ds(pl.multiple_of(channel * 8, 8), 8)
        rolled = [
            pltpu.roll(spread[first + i, rows, :], lax.rem(128 - rest, 128), 1) for i in range(count + 1)
        ]
        keep = lane < 128 - rest
        return [jnp.where(keep, rolled[i], rolled[i + 1]) for i in range(count)]

    def pair(i, carry):
        left, right = windows(2 * i), windows(2 * i + 1)
        for x in range(4):
            for l in range(WIN):
                value = jnp.concatenate([left[4 * x + l], right[4 * x + l]], axis=0)
                store(x, i // 2, l, lax.rem(i, 2) * 16, value.astype(jnp.bfloat16))
        return carry

    lax.fori_loop(0, 8, pair, 0)


def fine_kernel(step_ref, low_ref, got_ref, twist_ref, seg_ref, out_ref, turned, spread):
    beam = pl.program_id(0)

    @pl.when(beam == 0)
    def _():
        clear_pads(spread)

    fine_beam(lambda src, o, q: got_ref[src, 0, o, q], twist_ref, seg_ref, turned, spread, beam)

    @pl.when(beam == pl.num_programs(0) - 1)
    def _():
        def store(x, m, l, rows, value):
            out_ref[x, m, l, pl.ds(pl.multiple_of(rows, 16), 16), :] = value

        shifted_windows(step_ref[0], low_ref, spread, store)


def drift_kernel(got_ref, out_ref, rows, sums):
    steps = got_ref.shape[0]
    lane = lax.broadcasted_iota(jnp.int32, (8, 128), 1)
    for t in range(steps):
        for l in range(WIN):
            for pair in range(2):
                value = got_ref[t, l, pair * 16 : (pair + 1) * 16, :].astype(jnp.float32)
                rows[2 * pair, t, l] = value[0:8]
                rows[2 * pair + 1, t, l] = value[8:16]

    def channel(ch, carry):
        for j in range(NDRIFT):
            total = [None] * 4
            for t in range(steps):
                first, rest = (j * t) // 128, (j * t) % 128
                if rest == 0:
                    parts = [rows[ch, t, first + l] for l in range(4)]
                else:
                    rolled = [pltpu.roll(rows[ch, t, first + l], 128 - rest, 1) for l in range(5)]
                    parts = [
                        jnp.where(lane < 128 - rest, rolled[l], rolled[l + 1]) for l in range(4)
                    ]
                total = [p if s is None else s + p for s, p in zip(total, parts)]
            for l in range(4):
                sums[l, pl.ds(ch * 16 + j, 8, stride=STRIDE), :] = total[l] * (1.0 / steps)
        return carry

    lax.fori_loop(0, 4, channel, 0)
    for beam in range(8):
        for ch in range(4):
            start = beam * STRIDE + ch * 16
            for l in range(4):
                out_ref[beam, ch, :, l * 128 : (l + 1) * 128] = sums[l, start : start + 16, :]


def owner_z(pair, half, m):
    return 2 * m + half


def device_slots(pair, half, inner):
    m = jnp.arange(4, dtype=jnp.int32)
    owner = owner_z(pair, half, m) * 8 + inner
    return (owner[:, None] * 4 + jnp.arange(4, dtype=jnp.int32)[None, :]).reshape(16)


def shards(voltages, taps, busy_mask, drift_low):
    beams, lanes, seg, channels = voltages.shape
    tm_count = lax.axis_size("tm")
    chan_count = lax.axis_size("chan")
    tm, chan = lax.axis_index("tm"), lax.axis_index("chan")
    pair, pos = chan // SRC, chan % SRC
    step = (tm * (chan_count // SRC) + pair).astype(jnp.int32)

    total = tm_count * chan_count
    route = [(i + 1, i) for i in range(total - 1)]
    halo = lax.ppermute(voltages[:, :, :HALO], ("tm", "chan"), route)

    places = jnp.arange(SRC, dtype=jnp.int32)
    slots = jax.vmap(lambda d: device_slots(pair, d // 8, d % 8))(places).reshape(-1)
    before = jnp.cumsum(busy_mask) - busy_mask
    one_hot = (busy_mask[None, :] == 1) & (before[None, :] == slots[:, None])
    dft = jnp.dot(
        one_hot.astype(jnp.bfloat16), coarse_table(channels), preferred_element_type=jnp.float32
    ).astype(jnp.bfloat16)
    lows = jnp.sum(jnp.where(one_hot, drift_low[None, :], 0), axis=1).reshape(SRC, 16)
    low = jnp.sum(jnp.where(places[:, None] == pos, lows, 0), axis=0)

    sent = pl.pallas_call(
        coarse_kernel,
        grid=(beams,),
        in_specs=[
            pl.BlockSpec((1, 4, seg, channels), lambda b: (b, 0, 0, 0)),
            pl.BlockSpec((1, 4, HALO, channels), lambda b: (b, 0, 0, 0)),
            pl.BlockSpec(taps.shape, lambda b: (0, 0)),
            pl.BlockSpec(dft.shape, lambda b: (0, 0)),
        ],
        out_specs=pl.BlockSpec((SRC, 1, 2, 2, 16, SEG), lambda b: (0, b, 0, 0, 0, 0)),
        out_shape=jax.ShapeDtypeStruct((SRC, beams, 2, 2, 16, SEG), jnp.bfloat16),
        scratch_shapes=[
            pltpu.VMEM((channels // 128, SEG + HALO, 128), jnp.float32),
            pltpu.VMEM((2 * SEG, 2 * channels), jnp.bfloat16),
        ],
        compiler_params=pltpu.CompilerParams(vmem_limit_bytes=VMEM_LIMIT),
    )(voltages, halo, taps, dft)

    groups = [[g * SRC + i for i in range(SRC)] for g in range(chan_count // SRC)]
    got = lax.all_to_all(sent, "chan", 0, 0, axis_index_groups=groups, tiled=True)

    windows = pl.pallas_call(
        fine_kernel,
        grid=(beams,),
        in_specs=[
            pl.BlockSpec(memory_space=pltpu.SMEM),
            pl.BlockSpec(memory_space=pltpu.SMEM),
            pl.BlockSpec((SRC, 1, 2, 2, 16, SEG), lambda b: (0, b, 0, 0, 0, 0)),
            pl.BlockSpec((2, SRC, SEG), lambda b: (0, 0, 0)),
            pl.BlockSpec((2 * SEG, 2 * SEG), lambda b: (0, 0)),
        ],
        out_specs=pl.BlockSpec((4, 4, WIN, 32, 128), lambda b: (0, 0, 0, 0, 0)),
        out_shape=jax.ShapeDtypeStruct((4, 4, WIN, 32, 128), jnp.bfloat16),
        scratch_shapes=[
            pltpu.VMEM((2 * SRC * 16, 2 * SEG), jnp.bfloat16),
            pltpu.VMEM((BLOCKS, 128, 128), jnp.float32),
        ],
        compiler_params=pltpu.CompilerParams(vmem_limit_bytes=VMEM_LIMIT),
    )(step[None], low, got, twist_table(), segment_table())

    over_tm = lax.all_to_all(windows, "tm", 0, 0, tiled=True)
    groups = [[i + g * SRC for g in range(chan_count // SRC)] for i in range(SRC)]
    mine = lax.all_to_all(over_tm, "chan", 1, 1, axis_index_groups=groups, tiled=True)
    steps = mine.reshape(tm_count * (chan_count // SRC), WIN, 32, 128)

    return pl.pallas_call(
        drift_kernel,
        out_shape=jax.ShapeDtypeStruct((beams, 4, NDRIFT, BINS), jnp.float32),
        in_specs=[pl.BlockSpec(memory_space=pltpu.VMEM)],
        out_specs=pl.BlockSpec(memory_space=pltpu.VMEM),
        scratch_shapes=[
            pltpu.VMEM((4, steps.shape[0], WIN, 8, 128), jnp.float32),
            pltpu.VMEM((4, 8 * STRIDE, 128), jnp.float32),
        ],
        compiler_params=pltpu.CompilerParams(vmem_limit_bytes=VMEM_LIMIT),
    )(steps)


def solution(mesh):
    in_specs = (P(None, None, ("tm", "chan"), None), P(), P(), P())
    out_specs = P(None, "chan", None, "tm")
    return jax.shard_map(shards, mesh=mesh, in_specs=in_specs, out_specs=out_specs, check_vma=False)
```

```python
import math

import jax
import jax.numpy as jnp
import numpy as np
from jax import lax
from jax.experimental import pallas as pl
from jax.experimental.pallas import tpu as pltpu
from jax.sharding import PartitionSpec as P

TAPS = 4
NDRIFT = 16
SRC = 16
SEG = 128
FINE = SRC * SEG
HALO = 8
BINS = 512
MESH = pl.DeviceIdType.MESH
WIN = BINS // SEG + 2
PAD = 2
BLOCKS = PAD + SRC + 6
STRIDE = 72
VMEM_LIMIT = 60 * 1024 * 1024


def coarse_table(channels):
    n = np.arange(channels, dtype=np.int64)
    angle = ((n[:, None] * n[None, :]) % channels) * (2.0 * math.pi / channels)
    cos, sin = np.cos(angle), np.sin(angle)
    table = np.concatenate([cos, sin, -sin, cos], axis=1)
    return jnp.asarray(table.astype(np.float32)).astype(jnp.bfloat16)


def segment_table():
    s = np.arange(SEG, dtype=np.int64)
    lane = np.arange(SEG, dtype=np.int64)
    g = (lane % 16) * 8 + lane // 16
    angle = ((s[:, None] * g[None, :]) % SEG) * (2.0 * math.pi / SEG)
    cos, sin = np.cos(angle), np.sin(angle)
    table = np.concatenate(
        [np.concatenate([cos, -sin], axis=1), np.concatenate([sin, cos], axis=1)], axis=0
    )
    return jnp.asarray(table.astype(np.float32)).astype(jnp.bfloat16)


def twist_table():
    f = np.arange(SRC, dtype=np.int64)
    s = np.arange(SEG, dtype=np.int64)
    angle = ((f[:, None] * s[None, :]) % FINE) * (2.0 * math.pi / FINE)
    return jnp.asarray(np.stack([np.cos(angle), np.sin(angle)]).astype(np.float32))


def quarter_turns(value, count):
    re, im = value
    count %= 4
    if count == 0:
        return re, im
    if count == 1:
        return im, -re
    if count == 2:
        return -re, -im
    return -im, re


def turned_by(value, cos, sin):
    re, im = value
    return re * cos + im * sin, im * cos - re * sin


def added(left, right):
    return left[0] + right[0], left[1] + right[1]


def dropped(left, right):
    return left[0] - right[0], left[1] - right[1]


def dft4(values):
    a = added(values[0], values[2])
    b = dropped(values[0], values[2])
    c = added(values[1], values[3])
    d = quarter_turns(dropped(values[1], values[3]), 1)
    return [added(a, c), added(b, d), dropped(a, c), dropped(b, d)]


def filter_beam(volt, halo, taps_ref, ext, filt):
    tiles = ext.shape[0]
    for entry in range(4):
        o, p = entry // 2, entry % 2
        rows = volt(entry).astype(jnp.float32)
        tail = halo(entry).astype(jnp.float32)
        for l in range(tiles):
            lanes = slice(l * 128, (l + 1) * 128)
            ext[l, 0:SEG, :] = rows[:, lanes]
            ext[l, SEG : SEG + HALO, :] = tail[:, lanes]
        for l in range(tiles):
            lanes = slice(l * 128, (l + 1) * 128)
            total = taps_ref[0:1, lanes] * ext[l, 0:SEG, :]
            for tap in range(1, TAPS):
                total = total + taps_ref[tap : tap + 1, lanes] * ext[l, tap : tap + SEG, :]
            column = (p * tiles + l) * 128
            filt[o * SEG : (o + 1) * SEG, column : column + 128] = total.astype(jnp.bfloat16)


def coarse_of(filt, dft_ref, q, scale):
    depth = filt.shape[1]
    weights = dft_ref[:, q * depth : (q + 1) * depth]
    out = lax.dot_general(
        weights, filt[...], (((1,), (1,)), ((), ())), preferred_element_type=jnp.float32
    )
    return (out * scale).astype(jnp.bfloat16)


def fine_beam(load, twist_ref, seg_ref, turned, spread, beam):
    for o in range(2):
        inner = []
        for b in range(4):
            group = []
            for a in range(4):
                src = 4 * a + b
                group.append(
                    (load(src, o, 0).astype(jnp.float32), load(src, o, 1).astype(jnp.float32))
                )
            row = dft4(group)
            for f0 in range(1, 4):
                if b:
                    angle = 2.0 * math.pi * b * f0 / 16
                    row[f0] = turned_by(row[f0], math.cos(angle), math.sin(angle))
            inner.append(row)
        for f0 in range(4):
            outs = dft4([inner[b][f0] for b in range(4)])
            for f1 in range(4):
                f = f0 + 4 * f1
                value = outs[f1]
                if f:
                    value = turned_by(value, twist_ref[0, f : f + 1, :], twist_ref[1, f : f + 1, :])
                rows = slice((o * SRC + f) * 16, (o * SRC + f + 1) * 16)
                turned[rows, 0:SEG] = value[0].astype(jnp.bfloat16)
                turned[rows, SEG : 2 * SEG] = value[1].astype(jnp.bfloat16)
    lane = lax.broadcasted_iota(jnp.int32, (8, 128), 1)
    power = None
    for o in range(2):
        second = jnp.dot(
            turned[o * 256 : (o + 1) * 256, :], seg_ref[...], preferred_element_type=jnp.float32
        )
        re, im = second[:, 0:SEG], second[:, SEG : 2 * SEG]
        squares = re * re + im * im
        power = squares if power is None else power + squares
    power = power * (1.0 / (4.0 * FINE))
    for half in range(2):
        blocks = [power[f * 16 + half * 8 : f * 16 + half * 8 + 8, :] for f in range(SRC)]
        for bit in range(4):
            shift = 1 << bit
            upper = (lane & shift) != 0
            for f in range(SRC):
                if f & shift:
                    continue
                low, high = blocks[f], blocks[f | shift]
                blocks[f] = jnp.where(upper, pltpu.roll(high, shift, 1), low)
                blocks[f | shift] = jnp.where(upper, high, pltpu.roll(low, 128 - shift, 1))
        for h in range(SRC):
            spread[PAD + h, pl.ds(half * 64 + beam, 8, stride=8), :] = blocks[h]


def clear_pads(spread):
    zero = jnp.zeros((128, 128), jnp.float32)
    for h in range(PAD):
        spread[h] = zero
    for h in range(PAD + SRC, BLOCKS):
        spread[h] = zero


def shifted_windows(step, low_ref, spread, store):
    lane = lax.broadcasted_iota(jnp.int32, (8, 128), 1)
    count = 4 * 3 + WIN

    def windows(channel):
        start = low_ref[channel] * step + PAD * 128
        first = start // 128
        rest = start - first * 128
        rows = pl.ds(pl.multiple_of(channel * 8, 8), 8)
        rolled = [
            pltpu.roll(spread[first + i, rows, :], lax.rem(128 - rest, 128), 1) for i in range(count + 1)
        ]
        keep = lane < 128 - rest
        return [jnp.where(keep, rolled[i], rolled[i + 1]) for i in range(count)]

    def pair(i, carry):
        left, right = windows(2 * i), windows(2 * i + 1)
        for x in range(4):
            for l in range(WIN):
                value = jnp.concatenate([left[4 * x + l], right[4 * x + l]], axis=0)
                store(x, i // 2, l, lax.rem(i, 2) * 16, value.astype(jnp.bfloat16))
        return carry

    lax.fori_loop(0, 8, pair, 0)


def drift_sums(got, rows, sums, out_ref):
    steps = got.shape[0]
    lane = lax.broadcasted_iota(jnp.int32, (8, 128), 1)

    def widen(t, carry):
        for l in range(WIN):
            for pair in range(2):
                value = got[t, l, pair * 16 : (pair + 1) * 16, :].astype(jnp.float32)
                rows[2 * pair, t, l] = value[0:8]
                rows[2 * pair + 1, t, l] = value[8:16]
        return carry

    lax.fori_loop(0, steps, widen, 0)

    def channel(ch, carry):
        for j in range(NDRIFT):
            total = [None] * 4
            for t in range(steps):
                first, rest = (j * t) // 128, (j * t) % 128
                if rest == 0:
                    parts = [rows[ch, t, first + l] for l in range(4)]
                else:
                    rolled = [pltpu.roll(rows[ch, t, first + l], 128 - rest, 1) for l in range(5)]
                    parts = [
                        jnp.where(lane < 128 - rest, rolled[l], rolled[l + 1]) for l in range(4)
                    ]
                total = [p if s is None else s + p for s, p in zip(total, parts)]
            for l in range(4):
                sums[l, pl.ds(ch * 16 + j, 8, stride=STRIDE), :] = total[l] * (1.0 / steps)
        return carry

    lax.fori_loop(0, 4, channel, 0)
    for beam in range(8):
        for ch in range(4):
            start = beam * STRIDE + ch * 16
            for l in range(4):
                out_ref[beam, ch, :, l * 128 : (l + 1) * 128] = sums[l, start : start + 16, :]


def search_kernel(
    low_ref,
    volt_ref,
    halo_ref,
    taps_ref,
    dft_ref,
    twist_ref,
    seg_ref,
    out_ref,
    volt,
    ext,
    filt,
    sent,
    got,
    turned,
    spread,
    packed,
    taken,
    rows,
    sums,
    volt_sem,
    sent_sem,
    got_sem,
    packed_sem,
    taken_sem,
):
    beams = volt_ref.shape[0]
    tm, chan = lax.axis_index("tm"), lax.axis_index("chan")
    tm_count, pairs = lax.axis_size("tm"), lax.axis_size("chan") // SRC
    pair, pos = lax.div(chan, SRC), lax.rem(chan, SRC)
    half, inner = lax.div(pos, 8), lax.rem(pos, 8)
    step = tm * pairs + pair
    steps = taken.shape[0]

    def load(b):
        return pltpu.make_async_copy(volt_ref.at[b], volt.at[b], volt_sem.at[b])

    for b in range(beams):
        load(b).start()

    barrier = pltpu.get_barrier_semaphore()

    def greet_peer(off, carry):
        peer = pair * SRC + lax.rem(pos + off, SRC)
        pl.semaphore_signal(barrier, inc=1, device_id={"tm": tm, "chan": peer}, device_id_type=MESH)
        return carry

    lax.fori_loop(1, SRC, greet_peer, 0)
    for dx in range(4):
        for i in range(4):
            if dx or i:
                giver = source_chan(pair, half, inner, i)
                pl.semaphore_signal(
                    barrier,
                    inc=1,
                    device_id={"tm": lax.rem(tm + dx, 4), "chan": giver},
                    device_id_type=MESH,
                )
    clear_pads(spread)

    def exchange(b, source, place, off):
        peer = lax.rem(pos + off, SRC)
        return pltpu.make_async_remote_copy(
            src_ref=sent.at[source, b],
            dst_ref=got.at[place, b],
            send_sem=sent_sem.at[b, off],
            recv_sem=got_sem.at[b, place],
            device_id={"tm": tm, "chan": pair * SRC + peer},
            device_id_type=MESH,
        )

    scale = taps_ref.shape[1] ** -0.5

    def front(b, carry):
        load(b).wait()
        filter_beam(lambda i: volt[b, i], lambda i: halo_ref[b, i], taps_ref, ext, filt)
        for q in range(2):
            block = coarse_of(filt, dft_ref, q, scale)
            for d in range(SRC):
                for o in range(2):
                    sent[d, b, o, q] = block[d * 16 : (d + 1) * 16, o * SEG : (o + 1) * SEG]
        got[pos, b] = sent[pos, b]

        @pl.when(b == 0)
        def _():
            pl.semaphore_wait(barrier, 2 * SRC - 2)

        def send(off, carry):
            exchange(b, lax.rem(pos + off, SRC), pos, off).start()
            return carry

        lax.fori_loop(1, SRC, send, 0)
        return carry

    lax.fori_loop(0, beams, front, 0)

    def back(b, carry):
        def arrive(off, carry):
            peer = lax.rem(pos + off, SRC)
            exchange(b, peer, peer, off).wait_recv()
            return carry

        lax.fori_loop(1, SRC, arrive, 0)
        fine_beam(lambda src, o, q: got[src, b, o, q], twist_ref, seg_ref, turned, spread, b)
        return carry

    lax.fori_loop(0, beams, back, 0)

    def store(x, m, l, start, value):
        packed[x, m, l, pl.ds(pl.multiple_of(start, 16), 16), :] = value

    shifted_windows(step, low_ref, spread, store)

    def hand_over(dx, m):
        x = lax.rem(tm + dx, 4)
        return pltpu.make_async_remote_copy(
            src_ref=packed.at[x, m],
            dst_ref=taken.at[step],
            send_sem=packed_sem.at[dx, m],
            recv_sem=taken_sem.at[step],
            device_id={"tm": x, "chan": owner_z(pair, half, m) * 8 + inner},
            device_id_type=MESH,
        )

    for dx in range(4):
        for m in range(4):
            if dx or m:
                hand_over(dx, m).start()
    taken[step] = packed[tm, 0]

    def collect(off, carry):
        place = lax.rem(step + off, steps)
        pltpu.make_async_remote_copy(
            src_ref=packed.at[0, 0],
            dst_ref=taken.at[place],
            send_sem=packed_sem.at[0, 0],
            recv_sem=taken_sem.at[place],
            device_id={"tm": tm, "chan": pair * SRC + lax.rem(pos + 1, SRC)},
            device_id_type=MESH,
        ).wait_recv()
        return carry

    lax.fori_loop(1, steps, collect, 0)
    drift_sums(taken, rows, sums, out_ref)

    def finish(b, carry):
        def one(off, carry):
            exchange(b, lax.rem(pos + off, SRC), pos, off).wait_send()
            return carry

        return lax.fori_loop(1, SRC, one, carry)

    lax.fori_loop(0, beams, finish, 0)
    for dx in range(4):
        for m in range(4):
            if dx or m:
                hand_over(dx, m).wait_send()


def owner_z(pair, half, m):
    return lax.rem(2 * pair + half + (2 * half - 1) * m + 8, 8)


def source_chan(pair, half, inner, i):
    if i == 0:
        z = 2 * pair + half
    elif i == 1:
        z = 2 * pair + half + 2 - 4 * half + 8
    elif i == 2:
        z = 2 * pair + half - 1 + 2 * half + 8
    else:
        z = 2 * pair + half - 3 + 6 * half + 8
    return lax.rem(z, 8) * 8 + inner


def device_slots(pair, half, inner):
    m = jnp.arange(4, dtype=jnp.int32)
    owner = owner_z(pair, half, m) * 8 + inner
    return (owner[:, None] * 4 + jnp.arange(4, dtype=jnp.int32)[None, :]).reshape(16)


def shards(voltages, taps, busy_mask, drift_low):
    beams, lanes, seg, channels = voltages.shape
    tm_count = lax.axis_size("tm")
    chan_count = lax.axis_size("chan")
    tm, chan = lax.axis_index("tm"), lax.axis_index("chan")
    pair, pos = chan // SRC, chan % SRC

    total = tm_count * chan_count
    route = [(i + 1, i) for i in range(total - 1)]
    halo = lax.ppermute(voltages[:, :, :HALO], ("tm", "chan"), route)

    places = jnp.arange(SRC, dtype=jnp.int32)
    slots = jax.vmap(lambda d: device_slots(pair, d // 8, d % 8))(places).reshape(-1)
    before = jnp.cumsum(busy_mask) - busy_mask
    one_hot = (busy_mask[None, :] == 1) & (before[None, :] == slots[:, None])
    dft = jnp.dot(
        one_hot.astype(jnp.bfloat16), coarse_table(channels), preferred_element_type=jnp.float32
    ).astype(jnp.bfloat16)
    lows = jnp.sum(jnp.where(one_hot, drift_low[None, :], 0), axis=1).reshape(SRC, 16)
    low = jnp.sum(jnp.where(places[:, None] == pos, lows, 0), axis=0)

    steps = tm_count * (chan_count // SRC)
    vmem = pl.BlockSpec(memory_space=pltpu.VMEM)
    return pl.pallas_call(
        search_kernel,
        out_shape=jax.ShapeDtypeStruct((beams, 4, NDRIFT, BINS), jnp.float32),
        in_specs=[
            pl.BlockSpec(memory_space=pltpu.SMEM),
            pl.BlockSpec(memory_space=pl.ANY),
            vmem,
            vmem,
            vmem,
            vmem,
            vmem,
        ],
        out_specs=vmem,
        scratch_shapes=[
            pltpu.VMEM((beams, 4, seg, channels), jnp.bfloat16),
            pltpu.VMEM((channels // 128, SEG + HALO, 128), jnp.float32),
            pltpu.VMEM((2 * SEG, 2 * channels), jnp.bfloat16),
            pltpu.VMEM((SRC, beams, 2, 2, 16, SEG), jnp.bfloat16),
            pltpu.VMEM((SRC, beams, 2, 2, 16, SEG), jnp.bfloat16),
            pltpu.VMEM((2 * SRC * 16, 2 * SEG), jnp.bfloat16),
            pltpu.VMEM((BLOCKS, 128, 128), jnp.float32),
            pltpu.VMEM((4, 4, WIN, 32, 128), jnp.bfloat16),
            pltpu.VMEM((steps, WIN, 32, 128), jnp.bfloat16),
            pltpu.VMEM((4, steps, WIN, 8, 128), jnp.float32),
            pltpu.VMEM((4, 8 * STRIDE, 128), jnp.float32),
            pltpu.SemaphoreType.DMA((beams,)),
            pltpu.SemaphoreType.DMA((beams, SRC)),
            pltpu.SemaphoreType.DMA((beams, SRC)),
            pltpu.SemaphoreType.DMA((4, 4)),
            pltpu.SemaphoreType.DMA((steps,)),
        ],
        compiler_params=pltpu.CompilerParams(
            vmem_limit_bytes=VMEM_LIMIT, collective_id=0, has_side_effects=True
        ),
    )(low, voltages, halo, taps, dft, twist_table(), segment_table())


def solution(mesh):
    in_specs = (P(None, None, ("tm", "chan"), None), P(), P(), P())
    out_specs = P(None, "chan", None, "tm")
    return jax.shard_map(shards, mesh=mesh, in_specs=in_specs, out_specs=out_specs, check_vma=False)
```

```python
import math

import jax
import jax.numpy as jnp
import numpy as np
from jax import lax
from jax.experimental import pallas as pl
from jax.experimental.pallas import tpu as pltpu
from jax.sharding import PartitionSpec as P

TAPS = 4
NDRIFT = 16
DSPAN = 16
SRC = 16
SEG = 128
FINE = SRC * SEG
HALO = 8
BINS = 512
MESH = pl.DeviceIdType.MESH
WIN = BINS // SEG + 2
PAD = 2
BLOCKS = PAD + SRC + 6
STRIDE = 24
CHUNK = 2
MIX = 8 // CHUNK
SETS = 4 // MIX
TILES = WIN * SETS // 2
SLOT = 8 + CHUNK
VMEM_LIMIT = 60 * 1024 * 1024


def coarse_table(channels):
    n = np.arange(channels, dtype=np.int64)
    angle = ((n[:, None] * n[None, :]) % channels) * (2.0 * math.pi / channels)
    cos, sin = np.cos(angle), np.sin(angle)
    table = np.concatenate([cos, sin], axis=1)
    return jnp.asarray(table.astype(np.float32)).astype(jnp.bfloat16)


def segment_table():
    s = np.arange(SEG, dtype=np.int64)
    lane = np.arange(SEG, dtype=np.int64)
    g = (lane % 16) * 8 + lane // 16
    angle = ((s[:, None] * g[None, :]) % SEG) * (2.0 * math.pi / SEG)
    cos, sin = np.cos(angle), np.sin(angle)
    table = np.concatenate(
        [np.concatenate([cos, -sin], axis=1), np.concatenate([sin, cos], axis=1)], axis=0
    )
    return jnp.asarray(table.astype(np.float32)).astype(jnp.bfloat16)


def twist_table():
    f = np.arange(SRC, dtype=np.int64)
    s = np.arange(SEG, dtype=np.int64)
    angle = ((f[:, None] * s[None, :]) % FINE) * (2.0 * math.pi / FINE)
    return jnp.asarray(np.stack([np.cos(angle), np.sin(angle)]).astype(np.float32))


def quarter_turns(value, count):
    re, im = value
    count %= 4
    if count == 0:
        return re, im
    if count == 1:
        return im, -re
    if count == 2:
        return -re, -im
    return -im, re


def turned_by(value, cos, sin):
    re, im = value
    return re * cos + im * sin, im * cos - re * sin


def added(left, right):
    return left[0] + right[0], left[1] + right[1]


def dropped(left, right):
    return left[0] - right[0], left[1] - right[1]


def dft4(values):
    a = added(values[0], values[2])
    b = dropped(values[0], values[2])
    c = added(values[1], values[3])
    d = quarter_turns(dropped(values[1], values[3]), 1)
    return [added(a, c), added(b, d), dropped(a, c), dropped(b, d)]


def filter_beam(volt, halo, taps_ref, ext, filt):
    tiles = ext.shape[0]
    for entry in range(4):
        o, p = entry // 2, entry % 2
        rows = volt(entry).astype(jnp.float32)
        tail = halo(entry).astype(jnp.float32)
        for l in range(tiles):
            lanes = slice(l * 128, (l + 1) * 128)
            ext[l, 0:SEG, :] = rows[:, lanes]
            ext[l, SEG : SEG + HALO, :] = tail[:, lanes]
        for l in range(tiles):
            lanes = slice(l * 128, (l + 1) * 128)
            total = taps_ref[0:1, lanes] * ext[l, 0:SEG, :]
            for tap in range(1, TAPS):
                total = total + taps_ref[tap : tap + 1, lanes] * ext[l, tap : tap + SEG, :]
            column = (p * tiles + l) * 128
            filt[o * SEG : (o + 1) * SEG, column : column + 128] = total.astype(jnp.bfloat16)


def coarse_of(filt, dft_ref, q, scale):
    depth = filt.shape[1]
    weights = dft_ref[:, q * depth : (q + 1) * depth]
    out = lax.dot_general(
        weights, filt[...], (((1,), (1,)), ((), ())), preferred_element_type=jnp.float32
    )
    return (out * scale).astype(jnp.bfloat16)


def fine_beam(load, twist_ref, seg_ref, turned, spread, beam):
    for o in range(2):
        inner = []
        for b in range(4):
            group = []
            for a in range(4):
                src = 4 * a + b
                group.append(
                    (load(src, o, 0).astype(jnp.float32), load(src, o, 1).astype(jnp.float32))
                )
            row = dft4(group)
            for f0 in range(1, 4):
                if b:
                    angle = 2.0 * math.pi * b * f0 / 16
                    row[f0] = turned_by(row[f0], math.cos(angle), math.sin(angle))
            inner.append(row)
        for f0 in range(4):
            outs = dft4([inner[b][f0] for b in range(4)])
            for f1 in range(4):
                f = f0 + 4 * f1
                value = outs[f1]
                if f:
                    value = turned_by(value, twist_ref[0, f : f + 1, :], twist_ref[1, f : f + 1, :])
                rows = slice((o * SRC + f) * 16, (o * SRC + f + 1) * 16)
                turned[rows, 0:SEG] = value[0].astype(jnp.bfloat16)
                turned[rows, SEG : 2 * SEG] = value[1].astype(jnp.bfloat16)
    lane = lax.broadcasted_iota(jnp.int32, (8, 128), 1)
    power = None
    for o in range(2):
        second = jnp.dot(
            turned[o * 256 : (o + 1) * 256, :], seg_ref[...], preferred_element_type=jnp.float32
        )
        re, im = second[:, 0:SEG], second[:, SEG : 2 * SEG]
        squares = re * re + im * im
        power = squares if power is None else power + squares
    power = power * (1.0 / (4.0 * FINE))
    for half in range(2):
        blocks = [power[f * 16 + half * 8 : f * 16 + half * 8 + 8, :] for f in range(SRC)]
        for bit in range(4):
            shift = 1 << bit
            upper = (lane & shift) != 0
            for f in range(SRC):
                if f & shift:
                    continue
                low, high = blocks[f], blocks[f | shift]
                blocks[f] = jnp.where(upper, pltpu.roll(high, shift, 1), low)
                blocks[f | shift] = jnp.where(upper, high, pltpu.roll(low, 128 - shift, 1))
        for h in range(SRC):
            spread[PAD + h, pl.ds(half * 8 * SLOT + beam, 8, stride=SLOT), :] = blocks[h]


def clear(spread):
    zero = jnp.zeros(spread.shape[1:], jnp.float32)

    def one(h, carry):
        spread[h] = zero
        return carry

    lax.fori_loop(0, BLOCKS, one, 0)


def shifted_windows(step, low_ref, spread, store):
    lane = lax.broadcasted_iota(jnp.int32, (8, 128), 1)
    row = lax.broadcasted_iota(jnp.int32, (8, 128), 0)
    count = 4 * 3 + WIN

    def windows(group, at):
        low = jnp.clip(low_ref[group * MIX + at, 0], -DSPAN, DSPAN)
        start = low * step + PAD * 128
        first = start // 128
        rest = start - first * 128
        base = group * MIX * SLOT + at * 8
        rows = pl.ds(pl.multiple_of(base, 8), 8)
        turn = lax.rem(128 - rest, 128)
        rolled = [pltpu.roll(spread[first + i, rows, :], turn, 1) for i in range(count + 1)]
        keep = lane < 128 - rest
        return [jnp.where(keep, rolled[i], rolled[i + 1]) for i in range(count)]

    def owner(m, carry):
        merged = []
        for part in range(SETS):
            group = m * SETS + part
            value = windows(group, MIX - 1)
            for at in range(MIX - 2, -1, -1):
                below = row < (at + 1) * CHUNK
                value = [jnp.where(below, a, b) for a, b in zip(windows(group, at), value)]
            merged.append(value)
        for x in range(4):
            vectors = [merged[part][4 * x + l] for l in range(WIN) for part in range(SETS)]
            for i in range(TILES):
                value = jnp.concatenate([vectors[2 * i], vectors[2 * i + 1]], axis=0)
                store(x, m, i, value.astype(jnp.bfloat16))
        return carry

    lax.fori_loop(0, 4, owner, 0)


def drift_sums(take, rows, sums, put):
    steps = rows.shape[0]
    lane = lax.broadcasted_iota(jnp.int32, (8, 128), 1)

    def widen(t, carry):
        for i in range(TILES):
            value = take(t, i).astype(jnp.float32)
            for at in range(2):
                l, part = divmod(2 * i + at, SETS)
                rows[t, l, part] = value[at * 8 : (at + 1) * 8]
        return carry

    lax.fori_loop(0, steps, widen, 0)
    for part in range(SETS):
        for j in range(NDRIFT):
            total = [None] * 4
            for t in range(steps):
                first, rest = (j * t) // 128, (j * t) % 128
                if rest == 0:
                    parts = [rows[t, first + l, part] for l in range(4)]
                else:
                    rolled = [pltpu.roll(rows[t, first + l, part], 128 - rest, 1) for l in range(5)]
                    parts = [
                        jnp.where(lane < 128 - rest, rolled[l], rolled[l + 1]) for l in range(4)
                    ]
                total = [p if s is None else s + p for s, p in zip(total, parts)]
            for l in range(4):
                sums[l, pl.ds(j, 8, stride=STRIDE), :] = total[l] * (1.0 / steps)
        for at in range(MIX):
            for b in range(CHUNK):
                start = (at * CHUNK + b) * STRIDE
                for l in range(4):
                    put(part * MIX + at, b, l, sums[l, start : start + NDRIFT, :])


def slot_of(pair, place, index):
    half, inner = place // 8, place % 8
    z = (2 * pair + half + (2 * half - 1) * (index // 4) + 8) % 8
    return (z * 8 + inner) * 4 + index % 4


def choose_channels(pair, pos, mask_ref, low_ref, table, dft, own_low):
    channels = mask_ref.shape[1]
    busy = mask_ref[...] == 1
    ahead = lax.broadcasted_iota(jnp.int32, (channels, channels), 0) < lax.broadcasted_iota(
        jnp.int32, (channels, channels), 1
    )
    before = jnp.dot(
        jnp.broadcast_to(jnp.where(busy, 1.0, 0.0), (8, channels)).astype(jnp.bfloat16),
        jnp.where(ahead, 1.0, 0.0).astype(jnp.bfloat16),
        preferred_element_type=jnp.float32,
    )[0:1].astype(jnp.int32)
    before = jnp.where(busy, before, -1)
    row = lax.broadcasted_iota(jnp.int32, (16 * SRC, 1), 0)
    chosen = before == slot_of(pair, row // 16, row % 16)
    one_hot = jnp.where(chosen, 1.0, 0.0).astype(jnp.bfloat16)
    cos = jnp.dot(one_hot, table[:, 0:channels], preferred_element_type=jnp.float32)
    sin = jnp.dot(one_hot, table[:, channels : 2 * channels], preferred_element_type=jnp.float32)
    dft[:, 0:channels] = cos.astype(jnp.bfloat16)
    dft[:, channels : 2 * channels] = sin.astype(jnp.bfloat16)
    dft[:, 2 * channels : 3 * channels] = (-sin).astype(jnp.bfloat16)
    dft[:, 3 * channels : 4 * channels] = cos.astype(jnp.bfloat16)
    row = lax.broadcasted_iota(jnp.int32, (16, 1), 0)
    mine = before == slot_of(pair, pos, row)
    low = jnp.sum(jnp.where(mine, low_ref[...].astype(jnp.float32), 0.0), axis=1, keepdims=True)
    own_low[...] = jnp.broadcast_to(low, own_low.shape).astype(jnp.int32)


def search_kernel(
    mask_ref,
    low_ref,
    volt_ref,
    taps_ref,
    table_ref,
    twist_ref,
    seg_ref,
    out_ref,
    volt,
    halo,
    table,
    dft,
    own_low,
    low_word,
    ext,
    filt,
    sent,
    got,
    turned,
    spread,
    packed,
    taken,
    rows,
    sums,
    result,
    volt_sem,
    table_sem,
    low_sem,
    out_sem,
    halo_sent,
    halo_got,
    sent_sem,
    got_sem,
    packed_sem,
    taken_sem,
):
    beams = volt_ref.shape[0]
    tm, chan = lax.axis_index("tm"), lax.axis_index("chan")
    tm_count, chan_count = lax.axis_size("tm"), lax.axis_size("chan")
    pairs, total = chan_count // SRC, tm_count * chan_count
    pair, pos = lax.div(chan, SRC), lax.rem(chan, SRC)
    half, inner = lax.div(pos, 8), lax.rem(pos, 8)
    step = tm * pairs + pair
    steps = rows.shape[0]
    pieces = beams // CHUNK

    def device(tm_at, chan_at):
        return {"tm": tm_at, "chan": chan_at}

    def along(distance):
        place = lax.rem(tm * chan_count + chan + distance + total, total)
        return device(lax.div(place, chan_count), lax.rem(place, chan_count))

    def load(b):
        return pltpu.make_async_copy(volt_ref.at[b], volt.at[b], volt_sem.at[b])

    load_table = pltpu.make_async_copy(table_ref, table, table_sem)
    load_table.start()
    for b in range(beams):
        load(b).start()

    barrier = pltpu.get_barrier_semaphore()

    def greet(at):
        pl.semaphore_signal(barrier, inc=1, device_id=at, device_id_type=MESH)

    def greet_peer(off, carry):
        greet(device(tm, pair * SRC + lax.rem(pos + off, SRC)))
        return carry

    greet(along(1))
    lax.fori_loop(1, SRC, greet_peer, 0)
    for dx in range(4):
        for i in range(4):
            if dx or i:
                greet(device(lax.rem(tm + dx, 4), source_chan(pair, half, inner, i)))

    def pass_rows(b):
        return pltpu.make_async_remote_copy(
            src_ref=volt_ref.at[b, :, pl.ds(0, HALO), :],
            dst_ref=halo.at[b],
            send_sem=halo_sent.at[b],
            recv_sem=halo_got.at[b],
            device_id=along(-1),
            device_id_type=MESH,
        )

    pl.semaphore_wait(barrier, 2 * SRC - 1)
    for b in range(beams):
        pass_rows(b).start()
    clear(spread)
    load_table.wait()
    choose_channels(pair, pos, mask_ref, low_ref, table, dft, own_low)
    fetch_low = pltpu.make_async_copy(own_low, low_word, low_sem)

    def exchange(b, source, place, off):
        peer = lax.rem(pos + off, SRC)
        return pltpu.make_async_remote_copy(
            src_ref=sent.at[source, b],
            dst_ref=got.at[place, b],
            send_sem=sent_sem.at[b, off],
            recv_sem=got_sem.at[b, place],
            device_id=device(tm, pair * SRC + peer),
            device_id_type=MESH,
        )

    scale = taps_ref.shape[1] ** -0.5
    ends = tm * chan_count + chan == total - 1

    def front(b, carry):
        load(b).wait()
        pass_rows(b).wait_recv()

        def tail(i):
            value = halo[b, i]
            return jnp.where(ends, jnp.zeros_like(value), value)

        filter_beam(lambda i: volt[b, i], tail, taps_ref, ext, filt)
        for q in range(2):
            block = coarse_of(filt, dft, q, scale)
            for d in range(SRC):
                for o in range(2):
                    sent[d, b, o, q] = block[d * 16 : (d + 1) * 16, o * SEG : (o + 1) * SEG]
        got[pos, b] = sent[pos, b]

        def send(off, carry):
            exchange(b, lax.rem(pos + off, SRC), pos, off).start()
            return carry

        lax.fori_loop(1, SRC, send, 0)
        return carry

    lax.fori_loop(0, beams, front, 0)
    fetch_low.start()
    fetch_low.wait()

    def hand_over(q, dx, m):
        x = lax.rem(tm + dx, 4)
        return pltpu.make_async_remote_copy(
            src_ref=packed.at[q, x, m],
            dst_ref=taken.at[q, step],
            send_sem=packed_sem.at[q, dx, m],
            recv_sem=taken_sem.at[q, step],
            device_id=device(x, owner_z(pair, half, m) * 8 + inner),
            device_id_type=MESH,
        )

    def write(q):
        beams_of = pl.ds(q * CHUNK, CHUNK)
        return pltpu.make_async_copy(result.at[beams_of], out_ref.at[beams_of], out_sem.at[q])

    def transform(q):
        def one(k, carry):
            b = q * CHUNK + k

            def arrive(off, carry):
                peer = lax.rem(pos + off, SRC)
                exchange(b, peer, peer, off).wait_recv()
                return carry

            lax.fori_loop(1, SRC, arrive, 0)
            fine_beam(
                lambda src, o, p: got[src, b, o, p], twist_ref, seg_ref, turned, spread, k
            )
            return carry

        lax.fori_loop(0, CHUNK, one, 0)

        def store(x, m, i, value):
            packed[q, x, m, i] = value

        shifted_windows(step, low_word, spread, store)
        for dx in range(4):
            for m in range(4):
                if dx or m:
                    hand_over(q, dx, m).start()
        taken[q, step] = packed[q, tm, 0]

    def collect(q):
        def one(off, carry):
            place = lax.rem(step + off, steps)
            pltpu.make_async_remote_copy(
                src_ref=packed.at[q, 0, 0],
                dst_ref=taken.at[q, place],
                send_sem=packed_sem.at[q, 0, 0],
                recv_sem=taken_sem.at[q, place],
                device_id=device(tm, pair * SRC + lax.rem(pos + 1, SRC)),
                device_id_type=MESH,
            ).wait_recv()
            return carry

        lax.fori_loop(1, steps, one, 0)

        def put(channel, b, l, value):
            result[q * CHUNK + b, channel, :, l * 128 : (l + 1) * 128] = value

        drift_sums(lambda t, i: taken[q, t, i], rows, sums, put)
        write(q).start()

    def back(q, carry):
        @pl.when(q < pieces)
        def _():
            transform(q)

        @pl.when(q > 0)
        def _():
            collect(q - 1)

        return carry

    lax.fori_loop(0, pieces + 1, back, 0)

    def finish(b, carry):
        def one(off, carry):
            exchange(b, lax.rem(pos + off, SRC), pos, off).wait_send()
            return carry

        pass_rows(b).wait_send()
        return lax.fori_loop(1, SRC, one, carry)

    lax.fori_loop(0, beams, finish, 0)

    def finish_piece(q, carry):
        for dx in range(4):
            for m in range(4):
                if dx or m:
                    hand_over(q, dx, m).wait_send()
        write(q).wait()
        return carry

    lax.fori_loop(0, pieces, finish_piece, 0)


def owner_z(pair, half, m):
    return lax.rem(2 * pair + half + (2 * half - 1) * m + 8, 8)


def source_chan(pair, half, inner, i):
    if i == 0:
        z = 2 * pair + half
    elif i == 1:
        z = 2 * pair + half + 2 - 4 * half + 8
    elif i == 2:
        z = 2 * pair + half - 1 + 2 * half + 8
    else:
        z = 2 * pair + half - 3 + 6 * half + 8
    return lax.rem(z, 8) * 8 + inner


def shards(voltages, taps, busy_mask, drift_low):
    beams, lanes, seg, channels = voltages.shape
    steps = lax.axis_size("tm") * (lax.axis_size("chan") // SRC)
    pieces = beams // CHUNK
    vmem = pl.BlockSpec(memory_space=pltpu.VMEM)
    hbm = pl.BlockSpec(memory_space=pl.ANY)
    dma = pltpu.SemaphoreType.DMA
    return pl.pallas_call(
        search_kernel,
        out_shape=jax.ShapeDtypeStruct((beams, 4, NDRIFT, BINS), jnp.float32),
        in_specs=[vmem, vmem, hbm, vmem, hbm, vmem, vmem],
        out_specs=hbm,
        scratch_shapes=[
            pltpu.VMEM((beams, 4, seg, channels), jnp.bfloat16),
            pltpu.VMEM((beams, 4, HALO, channels), jnp.bfloat16),
            pltpu.VMEM((channels, 2 * channels), jnp.bfloat16),
            pltpu.VMEM((16 * SRC, 4 * channels), jnp.bfloat16),
            pltpu.VMEM((16, 128), jnp.int32),
            pltpu.SMEM((16, 128), jnp.int32),
            pltpu.VMEM((channels // 128, SEG + HALO, 128), jnp.float32),
            pltpu.VMEM((2 * SEG, 2 * channels), jnp.bfloat16),
            pltpu.VMEM((SRC, beams, 2, 2, 16, SEG), jnp.bfloat16),
            pltpu.VMEM((SRC, beams, 2, 2, 16, SEG), jnp.bfloat16),
            pltpu.VMEM((2 * SRC * 16, 2 * SEG), jnp.bfloat16),
            pltpu.VMEM((BLOCKS, 16 * SLOT, 128), jnp.float32),
            pltpu.VMEM((pieces, 4, 4, TILES, 16, 128), jnp.bfloat16),
            pltpu.VMEM((pieces, steps, TILES, 16, 128), jnp.bfloat16),
            pltpu.VMEM((steps, WIN, SETS, 8, 128), jnp.float32),
            pltpu.VMEM((4, 8 * STRIDE, 128), jnp.float32),
            pltpu.VMEM((beams, 4, NDRIFT, BINS), jnp.float32),
            dma((beams,)),
            dma,
            dma,
            dma((pieces,)),
            dma((beams,)),
            dma((beams,)),
            dma((beams, SRC)),
            dma((beams, SRC)),
            dma((pieces, 4, 4)),
            dma((pieces, steps)),
        ],
        compiler_params=pltpu.CompilerParams(
            vmem_limit_bytes=VMEM_LIMIT, collective_id=0, has_side_effects=True
        ),
    )(
        busy_mask[None, :],
        drift_low[None, :],
        voltages,
        taps,
        coarse_table(channels),
        twist_table(),
        segment_table(),
    )


def solution(mesh):
    in_specs = (P(None, None, ("tm", "chan"), None), P(), P(), P())
    out_specs = P(None, "chan", None, "tm")
    return jax.shard_map(shards, mesh=mesh, in_specs=in_specs, out_specs=out_specs, check_vma=False)
```

```python
import math

import jax
import jax.numpy as jnp
import numpy as np
from jax import lax
from jax.experimental import pallas as pl
from jax.experimental.pallas import tpu as pltpu
from jax.sharding import PartitionSpec as P

TAPS = 4
DEPTH = 3
NDRIFT = 16
DSPAN = 16
SRC = 16
SEG = 128
FINE = SRC * SEG
HALO = 8
BINS = 512
MESH = pl.DeviceIdType.MESH
WIN = BINS // SEG + 2
PAD = 2
BLOCKS = PAD + SRC + 6
STRIDE = 24
VECTORS = WIN // 2
SLOT = 10
VMEM_LIMIT = 60 * 1024 * 1024


def coarse_table(channels):
    n = np.arange(channels, dtype=np.int64)
    angle = ((n[:, None] * n[None, :]) % channels) * (2.0 * math.pi / channels)
    cos, sin = np.cos(angle), np.sin(angle)
    table = np.concatenate([cos, sin], axis=1)
    return jnp.asarray(table.astype(np.float32)).astype(jnp.bfloat16)


def segment_table():
    s = np.arange(SEG, dtype=np.int64)
    lane = np.arange(SEG, dtype=np.int64)
    g = (lane % 16) * 8 + lane // 16
    angle = ((s[:, None] * g[None, :]) % SEG) * (2.0 * math.pi / SEG)
    cos, sin = np.cos(angle), np.sin(angle)
    table = np.concatenate(
        [np.concatenate([cos, -sin], axis=1), np.concatenate([sin, cos], axis=1)], axis=0
    )
    return jnp.asarray(table.astype(np.float32)).astype(jnp.bfloat16)


def twist_table():
    f = np.arange(SRC, dtype=np.int64)
    s = np.arange(SEG, dtype=np.int64)
    angle = ((f[:, None] * s[None, :]) % FINE) * (2.0 * math.pi / FINE)
    return jnp.asarray(np.stack([np.cos(angle), np.sin(angle)]).astype(np.float32))


def quarter_turns(value, count):
    re, im = value
    count %= 4
    if count == 0:
        return re, im
    if count == 1:
        return im, -re
    if count == 2:
        return -re, -im
    return -im, re


def turned_by(value, cos, sin):
    re, im = value
    return re * cos + im * sin, im * cos - re * sin


def added(left, right):
    return left[0] + right[0], left[1] + right[1]


def dropped(left, right):
    return left[0] - right[0], left[1] - right[1]


def dft4(values):
    a = added(values[0], values[2])
    b = dropped(values[0], values[2])
    c = added(values[1], values[3])
    d = quarter_turns(dropped(values[1], values[3]), 1)
    return [added(a, c), added(b, d), dropped(a, c), dropped(b, d)]


def filter_beam(volt, taps_ref, ext, filt):
    tiles = ext.shape[0]
    for entry in range(4):
        o, p = entry // 2, entry % 2
        rows = volt(entry).astype(jnp.float32)
        for l in range(tiles):
            ext[l, 0:SEG, :] = rows[:, l * 128 : (l + 1) * 128]
        for l in range(tiles):
            lanes = slice(l * 128, (l + 1) * 128)
            total = taps_ref[0:1, lanes] * ext[l, 0:SEG, :]
            for tap in range(1, TAPS):
                total = total + taps_ref[tap : tap + 1, lanes] * ext[l, tap : tap + SEG, :]
            column = (p * tiles + l) * 128
            filt[o * SEG : (o + 1) * SEG, column : column + 128] = total.astype(jnp.bfloat16)


def lead_rows(head, taps_ref, first):
    channels = taps_ref.shape[1]
    row = lax.broadcasted_iota(jnp.int32, (8, channels), 0)
    keep = row < TAPS - 1

    def beam_rows(b, p):
        both = []
        for o in range(2):
            rows = jnp.where(keep, head[b, 2 * o + p].astype(jnp.float32), 0.0)
            total = rows * taps_ref[TAPS - 1 : TAPS, :]
            for back in range(1, TAPS - 1):
                tap = TAPS - 1 - back
                total = total + pltpu.roll(rows * taps_ref[tap : tap + 1, :], back, 0)
            both.append(jnp.where(keep, total, 0.0))
        return both[0] + pltpu.roll(both[1], 4, 0)

    def one(i, carry):
        for p in range(2):
            value = jnp.concatenate([beam_rows(2 * i, p), beam_rows(2 * i + 1, p)], axis=0)
            value = value.astype(jnp.bfloat16)
            for copy in range(2):
                rows = pl.ds(pl.multiple_of(copy * 64 + i * 16, 16), 16)
                first[rows, p * channels : (p + 1) * channels] = value
        return carry

    lax.fori_loop(0, head.shape[0] // 2, one, 0)


def coarse_of(filt, dft_ref, q, scale):
    depth = filt.shape[1]
    weights = dft_ref[:, q * depth : (q + 1) * depth]
    out = lax.dot_general(
        weights, filt[...], (((1,), (1,)), ((), ())), preferred_element_type=jnp.float32
    )
    return out * scale


def fine_beam(load, twist_ref, seg_ref, turned, spread):
    for o in range(2):
        inner = []
        for b in range(4):
            group = []
            for a in range(4):
                src = 4 * a + b
                group.append(
                    (load(src, o, 0), load(src, o, 1))
                )
            row = dft4(group)
            for f0 in range(1, 4):
                if b:
                    angle = 2.0 * math.pi * b * f0 / 16
                    row[f0] = turned_by(row[f0], math.cos(angle), math.sin(angle))
            inner.append(row)
        for f0 in range(4):
            outs = dft4([inner[b][f0] for b in range(4)])
            for f1 in range(4):
                f = f0 + 4 * f1
                value = outs[f1]
                if f:
                    value = turned_by(value, twist_ref[0, f : f + 1, :], twist_ref[1, f : f + 1, :])
                rows = slice((o * SRC + f) * 16, (o * SRC + f + 1) * 16)
                turned[rows, 0:SEG] = value[0].astype(jnp.bfloat16)
                turned[rows, SEG : 2 * SEG] = value[1].astype(jnp.bfloat16)
    lane = lax.broadcasted_iota(jnp.int32, (8, 128), 1)
    power = None
    for o in range(2):
        second = jnp.dot(
            turned[o * 256 : (o + 1) * 256, :], seg_ref[...], preferred_element_type=jnp.float32
        )
        re, im = second[:, 0:SEG], second[:, SEG : 2 * SEG]
        squares = re * re + im * im
        power = squares if power is None else power + squares
    power = power * (1.0 / (4.0 * FINE))
    for half in range(2):
        blocks = [power[f * 16 + half * 8 : f * 16 + half * 8 + 8, :] for f in range(SRC)]
        for bit in range(4):
            shift = 1 << bit
            upper = (lane & shift) != 0
            for f in range(SRC):
                if f & shift:
                    continue
                low, high = blocks[f], blocks[f | shift]
                blocks[f] = jnp.where(upper, pltpu.roll(high, shift, 1), low)
                blocks[f | shift] = jnp.where(upper, high, pltpu.roll(low, 128 - shift, 1))
        for h in range(SRC):
            for odd in range(2):
                spread[PAD + h, pl.ds(half * 8 * SLOT + odd, 8, stride=SLOT), :] = blocks[h]


def clear(spread):
    zero = jnp.zeros(spread.shape[1:], jnp.float32)

    def one(h, carry):
        spread[h] = zero
        return carry

    lax.fori_loop(0, BLOCKS, one, 0)


def shifted_windows(step, low_ref, spread, store):
    lane = lax.broadcasted_iota(jnp.int32, (8, 128), 1)
    row = lax.broadcasted_iota(jnp.int32, (8, 128), 0)
    count = 4 * 3 + WIN

    def windows(m, at):
        low = jnp.clip(low_ref[m * 4 + at, 0], -DSPAN, DSPAN)
        start = low * step + PAD * 128
        first = start // 128
        rest = start - first * 128
        rows = pl.ds(pl.multiple_of(m * 4 * SLOT + at * 8, 8), 8)
        turn = lax.rem(128 - rest, 128)
        rolled = [pltpu.roll(spread[first + i, rows, :], turn, 1) for i in range(count + 1)]
        keep = lane < 128 - rest
        return [jnp.where(keep, rolled[i], rolled[i + 1]) for i in range(count)]

    def owner(m, carry):
        value = windows(m, 3)
        for at in range(2, -1, -1):
            below = row < (at + 1) * 2
            value = [jnp.where(below, a, b) for a, b in zip(windows(m, at), value)]
        odd = lax.rem(row, 2) == 1
        for x in range(4):
            for k in range(VECTORS):
                block = 4 * x + 2 * k
                store(x, m, k, jnp.where(odd, value[block + 1], value[block]).astype(jnp.bfloat16))
        return carry

    lax.fori_loop(0, 4, owner, 0)


def drift_sums(take, rows, sums, put):
    steps = rows.shape[0]
    lane = lax.broadcasted_iota(jnp.int32, (8, 128), 1)
    odd = lax.rem(lax.broadcasted_iota(jnp.int32, (8, 128), 0), 2) == 1

    def widen(t, carry):
        even = [take(t, k).astype(jnp.float32) for k in range(VECTORS)]
        for k in range(VECTORS):
            rows[t, 2 * k] = even[k]
            if k + 1 < VECTORS:
                rows[t, 2 * k + 1] = jnp.where(
                    odd, pltpu.roll(even[k + 1], 1, 0), pltpu.roll(even[k], 7, 0)
                )
        return carry

    lax.fori_loop(0, steps, widen, 0)
    for j in range(NDRIFT):
        total = [None] * 2
        for t in range(steps):
            first, rest = (j * t) // 128, (j * t) % 128
            parts = []
            for a in range(2):
                value = rows[t, 2 * a + first]
                if rest:
                    following = pltpu.roll(rows[t, 2 * a + first + 1], 128 - rest, 1)
                    value = jnp.where(
                        lane < 128 - rest, pltpu.roll(value, 128 - rest, 1), following
                    )
                parts.append(value)
            total = [p if s is None else s + p for s, p in zip(total, parts)]
        for a in range(2):
            sums[a, pl.ds(j, 8, stride=STRIDE), :] = total[a] * (1.0 / steps)
    for channel in range(4):
        for l in range(4):
            start = (channel * 2 + l % 2) * STRIDE
            put(channel, l, sums[l // 2, start : start + NDRIFT, :])


def slot_of(pair, place, index):
    half, inner = place // 8, place % 8
    z = (2 * pair + half + (2 * half - 1) * (index // 4) + 8) % 8
    return (z * 8 + inner) * 4 + index % 4


def choose_channels(pair, pos, mask_ref, low_ref, table, dft, own_low):
    channels = mask_ref.shape[1]
    busy = mask_ref[...] == 1
    ahead = lax.broadcasted_iota(jnp.int32, (channels, channels), 0) < lax.broadcasted_iota(
        jnp.int32, (channels, channels), 1
    )
    before = jnp.dot(
        jnp.broadcast_to(jnp.where(busy, 1.0, 0.0), (8, channels)).astype(jnp.bfloat16),
        jnp.where(ahead, 1.0, 0.0).astype(jnp.bfloat16),
        preferred_element_type=jnp.float32,
    )[0:1].astype(jnp.int32)
    before = jnp.where(busy, before, -1)
    row = lax.broadcasted_iota(jnp.int32, (16 * SRC, 1), 0)
    chosen = before == slot_of(pair, row // 16, row % 16)
    one_hot = jnp.where(chosen, 1.0, 0.0).astype(jnp.bfloat16)
    cos = jnp.dot(one_hot, table[:, 0:channels], preferred_element_type=jnp.float32)
    sin = jnp.dot(one_hot, table[:, channels : 2 * channels], preferred_element_type=jnp.float32)
    dft[:, 0:channels] = cos.astype(jnp.bfloat16)
    dft[:, channels : 2 * channels] = sin.astype(jnp.bfloat16)
    dft[:, 2 * channels : 3 * channels] = (-sin).astype(jnp.bfloat16)
    dft[:, 3 * channels : 4 * channels] = cos.astype(jnp.bfloat16)
    if own_low is None:
        return
    row = lax.broadcasted_iota(jnp.int32, (16, 1), 0)
    mine = before == slot_of(pair, pos, row)
    low = jnp.sum(jnp.where(mine, low_ref[...].astype(jnp.float32), 0.0), axis=1, keepdims=True)
    own_low[...] = jnp.broadcast_to(low, own_low.shape).astype(jnp.int32)


def search_kernel(
    mask_hbm,
    low_hbm,
    volt_ref,
    taps_hbm,
    table_hbm,
    twist_hbm,
    seg_hbm,
    out_ref,
    mask_ref,
    low_ref,
    taps_ref,
    table,
    twist_ref,
    seg_ref,
    volt,
    head,
    dft,
    lead_dft,
    own_low,
    low_word,
    ext,
    filt,
    sent,
    got,
    first,
    lead,
    leads,
    turned,
    spread,
    packed,
    taken,
    rows,
    sums,
    result,
    volt_sem,
    small_sem,
    low_sem,
    out_sem,
    lead_sent,
    lead_got,
    sent_sem,
    got_sem,
    packed_sem,
    taken_sem,
    ring_sem,
):
    beams = volt_ref.shape[0]
    tm, chan = lax.axis_index("tm"), lax.axis_index("chan")
    tm_count, chan_count = lax.axis_size("tm"), lax.axis_size("chan")
    pairs = chan_count // SRC
    pair, pos = lax.div(chan, SRC), lax.rem(chan, SRC)
    half, inner = lax.div(pos, 8), lax.rem(pos, 8)
    step = tm * pairs + pair
    steps = rows.shape[0]

    def device(tm_at, chan_at):
        return {"tm": tm_at, "chan": chan_at}

    def in_group(distance, place):
        group = lax.rem(step + distance + steps, steps)
        return device(lax.div(group, pairs), lax.rem(group, pairs) * SRC + place)

    def along_z(distance):
        z = lax.rem(2 * pair + half + distance + 8, 8)
        return device(tm, z * 8 + inner)

    def call(far):
        for side in range(2):
            pl.semaphore_signal(
                ring_sem.at[2 * far + side],
                inc=1,
                device_id=along_z((1 - 2 * side) * (far + 1)),
                device_id_type=MESH,
            )

    def hear(far):
        for side in range(2):
            pl.semaphore_wait(ring_sem.at[2 * far + side], 1)

    def load(b):
        return pltpu.make_async_copy(volt_ref.at[b], volt.at[b], volt_sem.at[b])

    small = [
        pltpu.make_async_copy(source, target, small_sem.at[i])
        for i, (source, target) in enumerate(
            [
                (mask_hbm, mask_ref),
                (low_hbm, low_ref),
                (table_hbm, table),
                (taps_hbm, taps_ref),
                (seg_hbm, seg_ref),
                (volt_ref.at[:, :, pl.ds(0, HALO), :], head),
                (twist_hbm, twist_ref),
            ]
        )
    ]
    for copy in small:
        copy.start()
    for b in range(beams):
        load(b).start()

    barrier = pltpu.get_barrier_semaphore()

    def greet(at):
        pl.semaphore_signal(barrier, inc=1, device_id=at, device_id_type=MESH)

    def greet_peer(off, carry):
        greet(device(tm, pair * SRC + lax.rem(pos + off, SRC)))
        return carry

    greet(in_group(1, 0))
    lax.fori_loop(1, SRC, greet_peer, 0)
    for dx in range(1, 4):
        greet(device(lax.rem(tm + dx, 4), chan))
    greet(along_z(2 * half - 1))

    heads = 1 - lax.div(pos + SRC - 1, SRC)
    clear(spread)
    for l in range(ext.shape[0]):
        ext[l, SEG : SEG + HALO, :] = jnp.zeros((HALO, 128), jnp.float32)
    for copy in small[0:3]:
        copy.wait()
    choose_channels(pair, pos, mask_ref, low_ref, table, dft, own_low)
    for copy in small[3:]:
        copy.wait()
    fetch_low = pltpu.make_async_copy(own_low, low_word, low_sem)
    fetch_low.start()
    pl.semaphore_wait(barrier, SRC - 1 + 3 + 1 + SRC * heads)
    call(0)

    def pass_lead(off, place, kind=1):
        return pltpu.make_async_remote_copy(
            src_ref=lead.at[lax.rem(pos + off, SRC)],
            dst_ref=leads.at[place],
            send_sem=lead_sent.at[kind],
            recv_sem=lead_got.at[kind],
            device_id=in_group(-heads, lax.rem(pos + off, SRC)),
            device_id_type=MESH,
        )

    before = lax.rem(pos + SRC - 1, SRC)

    def exchange(b, source, place, off):
        peer = lax.rem(pos + off, SRC)
        return pltpu.make_async_remote_copy(
            src_ref=sent.at[source, b],
            dst_ref=got.at[place, b],
            send_sem=sent_sem.at[b],
            recv_sem=got_sem.at[b],
            device_id=device(tm, pair * SRC + peer),
            device_id_type=MESH,
        )

    others = pl.ds(0, SRC - 1)
    peer_device = device(tm, pair * SRC + lax.rem(pos + 1, SRC))

    def exchange_all(b):
        return pltpu.make_async_remote_copy(
            src_ref=sent.at[others, b],
            dst_ref=got.at[others, b],
            send_sem=sent_sem.at[b],
            recv_sem=got_sem.at[b],
            device_id=peer_device,
            device_id_type=MESH,
        )

    def lead_all():
        return pltpu.make_async_remote_copy(
            src_ref=lead.at[others],
            dst_ref=leads.at[others],
            send_sem=lead_sent.at[1],
            recv_sem=lead_got.at[1],
            device_id=peer_device,
            device_id_type=MESH,
        )

    def hand_over_all(q):
        return pltpu.make_async_remote_copy(
            src_ref=taken.at[q, others],
            dst_ref=taken.at[q, others],
            send_sem=packed_sem.at[q],
            recv_sem=taken_sem.at[q],
            device_id=peer_device,
            device_id_type=MESH,
        )

    scale = taps_ref.shape[1] ** -0.5
    def leading():
        choose_channels(pair - heads, pos, mask_ref, low_ref, table, lead_dft, None)
        lead_rows(head, taps_ref, first)
        blocks = [coarse_of(first, lead_dft, q, scale) for q in range(2)]
        low_lanes = lax.broadcasted_iota(jnp.int32, blocks[0].shape, 1) < 64
        both = jnp.where(low_lanes, blocks[0], blocks[1])
        for d in range(SRC):
            lead[d] = both[d * 16 : (d + 1) * 16, :].astype(jnp.bfloat16)

        def send_lead(off, carry):
            pass_lead(off, before).start()
            return carry

        lax.fori_loop(1, SRC, send_lead, 0)

        @pl.when(heads == 1)
        def _():
            pass_lead(0, before, 0).start()

        @pl.when(heads == 0)
        def _():
            leads[before] = lead[pos]

    def front(b, carry):
        load(b).wait()
        filter_beam(lambda i: volt[b, i], taps_ref, ext, filt)
        for q in range(2):
            block = coarse_of(filt, dft, q, scale)
            for d in range(SRC):
                for o in range(2):
                    value = block[d * 16 : (d + 1) * 16, o * SEG : (o + 1) * SEG]
                    sent[d, b, o, q] = value.astype(jnp.bfloat16)
        got[pos, b] = sent[pos, b]

        def send(off, carry):
            exchange(b, lax.rem(pos + off, SRC), pos, off).start()
            return carry

        lax.fori_loop(1, SRC, send, 0)
        pl.when(b == 0)(leading)
        return carry

    lax.fori_loop(0, beams, front, 0)
    hear(0)
    call(1)
    fetch_low.wait()
    lane = lax.broadcasted_iota(jnp.int32, (16, SEG), 1)

    def arrived(b, src, o, p):
        value = got[src, b, o, p].astype(jnp.float32)
        extra = leads[src].astype(jnp.float32)
        turn = lax.rem(2 * SEG - (TAPS - 1) - p * 64 - (2 * b + o) * 4, SEG)
        start = SEG - (TAPS - 1)
        if src == SRC - 1:
            start = start + (TAPS - 1) * lax.div(step + 1, steps)
        return value + jnp.where(lane >= start, pltpu.roll(extra, turn, 1), 0.0)


    def hand_over(q, dx, m):
        x = lax.rem(tm + dx, 4)
        return pltpu.make_async_remote_copy(
            src_ref=packed.at[q, x, m],
            dst_ref=taken.at[q, step],
            send_sem=packed_sem.at[q],
            recv_sem=taken_sem.at[q],
            device_id=device(x, owner_z(pair, half, m) * 8 + inner),
            device_id_type=MESH,
        )

    def write(q):
        return pltpu.make_async_copy(result.at[q], out_ref.at[q], out_sem.at[q])

    def transform(q):
        exchange_all(q).wait_recv()
        fine_beam(lambda src, o, p: arrived(q, src, o, p), twist_ref, seg_ref, turned, spread)

        def store(x, m, k, value):
            packed[q, x, m, k] = value

        shifted_windows(step, low_word, spread, store)
        for m in range(3, -1, -1):
            for dx in (2, 1, 3, 0):
                if dx or m:
                    hand_over(q, dx, m).start()
        taken[q, step] = packed[q, tm, 0]

    def collect(q):
        hand_over_all(q).wait_recv()

        def put(channel, l, value):
            result[q, channel, :, l * 128 : (l + 1) * 128] = value

        drift_sums(lambda t, k: taken[q, t, k], rows, sums, put)
        write(q).start()

    lead_all().wait_recv()
    hear(1)

    @pl.when(heads == 1)
    def _():
        pass_lead(0, before, 0).wait_recv()

    def finish():
        def one(b, carry):
            exchange_all(b).wait_send()
            return carry

        lax.fori_loop(0, beams, one, 0)
        lead_all().wait_send()

        @pl.when(heads == 1)
        def _():
            pass_lead(0, before, 0).wait_send()

    def back(q, carry):
        @pl.when(q < beams)
        def _():
            transform(q)

        pl.when(q == beams)(finish)

        @pl.when(q >= DEPTH)
        def _():
            collect(q - DEPTH)

        return carry

    lax.fori_loop(0, beams + DEPTH, back, 0)

    def close(q, carry):
        hand_over_all(q).wait_send()
        write(q).wait()
        return carry

    lax.fori_loop(0, beams, close, 0)


def owner_z(pair, half, m):
    return lax.rem(2 * pair + half + (2 * half - 1) * m + 8, 8)


def shards(voltages, taps, busy_mask, drift_low):
    beams, lanes, seg, channels = voltages.shape
    steps = lax.axis_size("tm") * (lax.axis_size("chan") // SRC)
    hbm = pl.BlockSpec(memory_space=pl.ANY)
    dma = pltpu.SemaphoreType.DMA
    return pl.pallas_call(
        search_kernel,
        out_shape=jax.ShapeDtypeStruct((beams, 4, NDRIFT, BINS), jnp.float32),
        in_specs=[hbm] * 7,
        out_specs=hbm,
        scratch_shapes=[
            pltpu.VMEM((1, channels), jnp.int32),
            pltpu.VMEM((1, channels), jnp.int32),
            pltpu.VMEM(taps.shape, jnp.float32),
            pltpu.VMEM((channels, 2 * channels), jnp.bfloat16),
            pltpu.VMEM((2, SRC, SEG), jnp.float32),
            pltpu.VMEM((2 * SEG, 2 * SEG), jnp.bfloat16),
            pltpu.VMEM((beams, 4, seg, channels), jnp.bfloat16),
            pltpu.VMEM((beams, 4, HALO, channels), jnp.bfloat16),
            pltpu.VMEM((16 * SRC, 4 * channels), jnp.bfloat16),
            pltpu.VMEM((16 * SRC, 4 * channels), jnp.bfloat16),
            pltpu.VMEM((16, 128), jnp.int32),
            pltpu.SMEM((16, 128), jnp.int32),
            pltpu.VMEM((channels // 128, SEG + HALO, 128), jnp.float32),
            pltpu.VMEM((2 * SEG, 2 * channels), jnp.bfloat16),
            pltpu.VMEM((SRC, beams, 2, 2, 16, SEG), jnp.bfloat16),
            pltpu.VMEM((SRC, beams, 2, 2, 16, SEG), jnp.bfloat16),
            pltpu.VMEM((beams * 16, 2 * channels), jnp.bfloat16),
            pltpu.VMEM((SRC, 16, SEG), jnp.bfloat16),
            pltpu.VMEM((SRC, 16, SEG), jnp.bfloat16),
            pltpu.VMEM((2 * SRC * 16, 2 * SEG), jnp.bfloat16),
            pltpu.VMEM((BLOCKS, 16 * SLOT, 128), jnp.float32),
            pltpu.VMEM((beams, 4, 4, VECTORS, 8, 128), jnp.bfloat16),
            pltpu.VMEM((beams, steps, VECTORS, 8, 128), jnp.bfloat16),
            pltpu.VMEM((steps, WIN - 1, 8, 128), jnp.float32),
            pltpu.VMEM((2, 8 * STRIDE, 128), jnp.float32),
            pltpu.VMEM((beams, 4, NDRIFT, BINS), jnp.float32),
            dma((beams,)),
            dma((7,)),
            dma,
            dma((beams,)),
            dma((2,)),
            dma((2,)),
            dma((beams,)),
            dma((beams,)),
            dma((beams,)),
            dma((beams,)),
            pltpu.SemaphoreType.REGULAR((4,)),
        ],
        compiler_params=pltpu.CompilerParams(
            vmem_limit_bytes=VMEM_LIMIT, collective_id=0, has_side_effects=True
        ),
    )(
        busy_mask[None, :],
        drift_low[None, :],
        voltages,
        taps,
        coarse_table(channels),
        twist_table(),
        segment_table(),
    )


def solution(mesh):
    in_specs = (P(None, None, ("tm", "chan"), None), P(), P(), P())
    out_specs = P(None, "chan", None, "tm")
    return jax.shard_map(shards, mesh=mesh, in_specs=in_specs, out_specs=out_specs, check_vma=False)
```
